32 devices in a mesh: dp: 4 (over x, core), band: 8 (over z, y).
Axes of the slice: x: 2, y: 2, z: 4, core: 2. Of those that a mesh axis runs over, the one named last changes fastest.
Arguments:
- features: bfloat16 [8160, 256], P(('dp', 'band')), parts along dimension 0, may hold values from -6 to 6
- corners: int32 [8160, 512], P(('dp', 'band')), parts along dimension 0, may hold values from 0 to 1535, as said below
- bilinear: float32 [8160, 512], P(('dp', 'band')), parts along dimension 0, may hold values from 0.08 to 0.5, as said below
- attention: float32 [8160, 128], P(('dp', 'band')), parts along dimension 0, may hold values from 0 to 1, as said below
- w_value: bfloat16 [256, 256], replicated, may hold values from -0.375 to 0.375
- b_value: float32 [256], replicated, may hold values from -0.6 to 0.6
- w_out: bfloat16 [256, 256], replicated, may hold values from -1.5 to 1.5
- b_out: float32 [256], replicated, may hold values from -3 to 3
- norm1_gain: float32 [256], replicated, may hold values from 0.5 to 1.5
- norm1_bias: float32 [256], replicated, may hold values from -3 to 3
- w_in: bfloat16 [256, 1024], replicated, may hold values from -0.375 to 0.375
- b_in: float32 [1024], replicated, may hold values from -3 to 3
- w_ffout: bfloat16 [1024, 256], replicated, may hold values from -0.1875 to 0.1875
- b_ffout: float32 [256], replicated, may hold values from -3 to 3
- norm2_gain: float32 [256], replicated, may hold values from 0.5 to 1.5
- norm2_bias: float32 [256], replicated, may hold values from -3 to 3
Outputs:
- encoded: bfloat16 [8160, 256], P(('dp', 'band')), parts along dimension 0
The draws below stay inside these ranges and needn't reach their ends.
There are 4 independent parts, one for each index of `dp`. The reference program is written for one: setup_inputs(seed, part) draws one part's arguments, and reference() takes and returns one part's arrays. A program takes and returns all parts, laid end to end along the dimension named above; an argument that names none is the same for every part. Nothing has to cross between parts.
Inputs may be any that keep to these rules, and one draw needn't show every extreme that they name: An entry for level l is a row of a map of 192 * 8 // 4**l tokens laid out in rows of 128 // 2**l; the four corners of a point are k, k + 1, k + 128 // 2**l and k + 128 // 2**l + 1 in that order. `bilinear`: the four corner weights of a point are positive and sum to one. `attention`: for each token and head the 16 weights are positive and sum to one.
All inputs are finite; a program needn't handle non-finite values.
Results may differ from the reference program's by a relative error of at most 0.009.
Values may be sent and summed in bfloat16 or wider, within the bound.
A program may use at most 64 MiB of HBM per device.

```python
import jax
import jax.numpy as jnp
from jax import lax

D = 256
HEADS = 8
FF = 1024
LEVELS = 4
POINTS = 4
MAP_W = 128
ROWS_DEV = 192
BAND_ROWS = 255
TOKENS = 2040


def query_place():
    band_total = TOKENS // BAND_ROWS
    token_ids = jnp.arange(TOKENS, dtype=jnp.int32)
    band_index = token_ids // BAND_ROWS
    local_row = token_ids % BAND_ROWS
    own_position = band_index * ROWS_DEV + local_row
    own_length = jnp.zeros((TOKENS,), jnp.int32) + ROWS_DEV * band_total
    offset_rows = 0
    for level_index in range(LEVELS):
        rows_here = ROWS_DEV // 4 ** level_index
        inside = (local_row >= offset_rows) & (local_row < offset_rows + rows_here)
        own_position = jnp.where(inside, band_index * rows_here + local_row - offset_rows, own_position)
        own_length = jnp.where(inside, rows_here * band_total, own_length)
        offset_rows = offset_rows + rows_here
    return (own_position, own_length)


def draw_corners(key, part):
    band_total = TOKENS // BAND_ROWS
    own_position, own_length = query_place()
    tables = []
    for level_index in range(LEVELS):
        rows_here = ROWS_DEV // 4 ** level_index
        length = rows_here * band_total
        stride = MAP_W // 2 ** level_index
        shape_here = (TOKENS, HEADS, POINTS)
        keys_here = jax.random.split(jax.random.fold_in(key, 11 + level_index), 4)
        centre = (own_position * length // own_length)[:, None, None]
        jitter = jax.random.randint(keys_here[0], shape_here, -rows_here, rows_here + 1) + jax.random.randint(keys_here[1], shape_here, -rows_here, rows_here + 1)
        faraway = jax.random.randint(keys_here[2], shape_here, 0, length)
        choose = jax.random.randint(keys_here[3], shape_here, 0, 4) != 0
        anchor = jnp.clip(jnp.where(choose, faraway, centre + jitter), 0, length - stride - 2)
        tables.append(jnp.stack([anchor, anchor + 1, anchor + stride, anchor + stride + 1], axis=-1))
    return jnp.stack(tables, axis=2).reshape(TOKENS, HEADS * LEVELS * POINTS * 4).astype(jnp.int32)


def draw_bilinear(key, part):
    key_first, key_second = jax.random.split(jax.random.fold_in(key, 29))
    shape_here = (TOKENS, HEADS * LEVELS * POINTS)
    first = jax.random.uniform(key_first, shape_here, jnp.float32)
    second = jax.random.uniform(key_second, shape_here, jnp.float32)
    first = 0.3 + 0.4 * first
    second = 0.3 + 0.4 * second
    stacked = jnp.stack([(1.0 - first) * (1.0 - second), first * (1.0 - second), (1.0 - first) * second, first * second], axis=-1)
    return stacked.reshape(TOKENS, HEADS * LEVELS * POINTS * 4).astype(jnp.float32)


def draw_attention(key, part):
    key_logit = jax.random.fold_in(key, 37)
    shape_here = (TOKENS, HEADS, LEVELS * POINTS)
    finer = jnp.arange(LEVELS * POINTS, dtype=jnp.int32) // POINTS < 2
    noise = jax.random.normal(key_logit, shape_here, jnp.float32)
    logits = jnp.where(finer, 0.3 * noise, 1.35 + 0.8 * noise)
    return jax.nn.softmax(logits, axis=-1).reshape(TOKENS, HEADS * LEVELS * POINTS).astype(jnp.float32)


def block_scale(stream_key, shape, pieces, smallest, top_value):
    def one(axis_at, shards_of):
        steps = jax.random.uniform(jax.random.fold_in(jax.random.fold_in(stream_key, 6), axis_at), (shards_of,), jnp.float32, smallest / len(pieces), top_value / len(pieces))
        return jnp.repeat(jnp.exp(steps), shape[axis_at] // shards_of).reshape((-1,) + (1,) * (len(shape) - axis_at - 1))

    level = one(*pieces[0])
    for cut in pieces[1:]:
        level = level * one(*cut)
    return level


def bell_draw(rng, dims, deviation, limit, pieces=(), held_as=jnp.bfloat16):
    loudness = block_scale(rng, dims, pieces, -0.22, 0.18) if pieces else 1.0
    values = jax.random.normal(rng, dims, jnp.float32) * deviation * loudness
    return jnp.minimum(jnp.maximum(values, -limit), limit).astype(held_as)


def setup_inputs(seed: int = 0, part: int = 0) -> dict:
    key_list = jax.random.split(jax.random.key(seed), 17)
    own_keys = jax.random.split(jax.random.fold_in(key_list[16], part), 17)
    return {
        "features": bell_draw(own_keys[0], (TOKENS, D), 1.0, 6.0, ((0, 8),)),
        "corners": draw_corners(jax.random.fold_in(jax.random.fold_in(key_list[16], part), 71), part),
        "bilinear": draw_bilinear(jax.random.fold_in(jax.random.fold_in(key_list[16], part), 71), part),
        "attention": draw_attention(jax.random.fold_in(jax.random.fold_in(key_list[16], part), 71), part),
        "w_value": bell_draw(key_list[4], (D, D), D ** -0.5, 0.375),
        "b_value": bell_draw(key_list[5], (D,), 0.1, 0.6, (), jnp.float32),
        "w_out": bell_draw(key_list[6], (D, D), (D // 16) ** -0.5, 1.5),
        "b_out": bell_draw(key_list[7], (D,), 0.5, 3.0, (), jnp.float32),
        "norm1_gain": jnp.clip(1.0 + 0.1 * jax.random.normal(key_list[8], (D,), jnp.float32), 0.5, 1.5),
        "norm1_bias": bell_draw(key_list[9], (D,), 0.5, 3.0, (), jnp.float32),
        "w_in": bell_draw(key_list[10], (D, FF), D ** -0.5, 0.375),
        "b_in": bell_draw(key_list[11], (FF,), 0.5, 3.0, (), jnp.float32),
        "w_ffout": bell_draw(key_list[12], (FF, D), FF ** -0.5, 0.1875),
        "b_ffout": bell_draw(key_list[13], (D,), 0.5, 3.0, (), jnp.float32),
        "norm2_gain": jnp.clip(1.0 + 0.1 * jax.random.normal(key_list[14], (D,), jnp.float32), 0.5, 1.5),
        "norm2_bias": bell_draw(key_list[15], (D,), 0.5, 3.0, (), jnp.float32),
    }


def layer_norm(inputs, gain, shift):
    average = lax.optimization_barrier(jnp.mean(inputs, axis=-1, keepdims=True))
    centred = inputs - average
    variance = lax.optimization_barrier(jnp.mean(centred * centred, axis=-1, keepdims=True))
    return centred * lax.rsqrt(variance + 1e-05) * gain + shift

def reference(features, corners, bilinear, attention, w_value, b_value, w_out, b_out, norm1_gain, norm1_bias, w_in, b_in, w_ffout, b_ffout, norm2_gain, norm2_bias):
    token_count, model_width = features.shape
    head_dim = model_width // HEADS
    samples = LEVELS * POINTS * 4
    segment_rows = [ROWS_DEV // 4 ** level_index for level_index in range(LEVELS)]
    segment_start = [sum(segment_rows[:level_index]) for level_index in range(LEVELS)]
    value_rows = (jnp.dot(features, w_value, preferred_element_type=jnp.float32) + b_value).astype(jnp.bfloat16)
    weight = (attention.reshape(token_count, HEADS, LEVELS, POINTS, 1) * bilinear.reshape(token_count, HEADS, LEVELS, POINTS, 4)).astype(jnp.bfloat16)
    weight = weight.reshape(token_count, HEADS, samples)
    corner_table = corners.reshape(token_count, HEADS, LEVELS, POINTS * 4)
    places = []
    for level_index in range(LEVELS):
        level_corner = corner_table[:, :, level_index]
        places.append(level_corner // segment_rows[level_index] * BAND_ROWS + segment_start[level_index] + level_corner % segment_rows[level_index])
    place_table = jnp.stack(places, axis=2).reshape(token_count, HEADS, samples)
    flat_index = (place_table * HEADS + jnp.arange(HEADS, dtype=jnp.int32)[None, :, None]).astype(jnp.int32)
    flat_value = value_rows.reshape(token_count * HEADS, head_dim)
    band_count = token_count // BAND_ROWS

    def blend_block(block_args):
        index_block, weight_block = block_args
        picked = flat_value[index_block].astype(jnp.float32)
        return lax.optimization_barrier(jnp.sum(weight_block.astype(jnp.float32)[..., None] * picked, axis=2))
    sampled = lax.map(blend_block, (flat_index.reshape(band_count, BAND_ROWS, HEADS, samples), weight.reshape(band_count, BAND_ROWS, HEADS, samples)))
    sampled = sampled.reshape(token_count, model_width).astype(jnp.bfloat16)
    attended = jnp.dot(sampled, w_out, preferred_element_type=jnp.float32) + b_out
    middle = layer_norm(features.astype(jnp.float32) + attended, norm1_gain, norm1_bias).astype(jnp.bfloat16)
    hidden = jnp.maximum(jnp.dot(middle, w_in, preferred_element_type=jnp.float32) + b_in, 0.0).astype(jnp.bfloat16)
    result = middle.astype(jnp.float32) + jnp.dot(hidden, w_ffout, preferred_element_type=jnp.float32) + b_ffout
    return layer_norm(result, norm2_gain, norm2_bias).astype(jnp.bfloat16)
```

```python
import functools

import jax
import jax.numpy as jnp
from jax import lax
from jax.experimental import pallas as pl
from jax.experimental.pallas import tpu as pltpu
from jax.sharding import PartitionSpec as P

HEADS = 8
LEVELS = 4
POINTS = 4
ROWS_DEV = 192
MAP_W = 128
LANES = 128
UNIT = 16
CHUNK = 128
BUILT = (5, 9, 12, 14)

F32 = jnp.float32
BF16 = jnp.bfloat16
MESH = pl.DeviceIdType.MESH


def norm(inputs, gain, shift):
    average = jnp.mean(inputs, axis=-1, keepdims=True)
    centred = inputs - average
    variance = jnp.mean(centred * centred, axis=-1, keepdims=True)
    return centred * lax.rsqrt(variance + 1e-05) * gain + shift


def kernel(
    bands,
    feat_hbm,
    corners_hbm,
    bilinear_hbm,
    attention_hbm,
    w_value_hbm,
    b_value_hbm,
    w_out_hbm,
    b_out_hbm,
    gain1_hbm,
    bias1_hbm,
    w_in_hbm,
    b_in_hbm,
    w_ff_hbm,
    b_ff_hbm,
    gain2_hbm,
    bias2_hbm,
    out,
    gathered,
    corners,
    bilinear,
    attention,
    w_value,
    b_value,
    w_out,
    b_out,
    gain1,
    bias1,
    w_in,
    b_in,
    w_ff,
    b_ff,
    gain2,
    bias2,
    w_value_t,
    shift_t,
    turned_t,
    row_t,
    column_t,
    row_next_t,
    column_next_t,
    place_t,
    weight_t,
    matrix,
    samp_t,
    send_sem,
    recv_sem,
    load_sem,
):
    rows = [ROWS_DEV // 4**level for level in range(LEVELS)]
    starts = [sum(rows[:level]) for level in range(LEVELS)]
    widths = [MAP_W // 2**level for level in range(LEVELS)]
    tokens, model = feat_hbm.shape
    head_dim = model // HEADS
    padded = matrix.shape[3]
    halves = matrix.shape[2]
    points = HEADS * LEVELS * POINTS
    me = lax.axis_index("band")

    line = bands // 2
    mine_z, mine_y = me // 2, lax.rem(me, 2)
    partner = mine_z * 2 + 1 - mine_y
    has_left, has_right = mine_z > 0, mine_z < line - 1
    cuts = [(begin, min(begin + CHUNK, tokens) - begin) for begin in range(0, tokens, CHUNK)]

    barrier = pltpu.get_barrier_semaphore()

    def greet(target):
        pl.semaphore_signal(barrier, inc=1, device_id={"band": target}, device_id_type=MESH)

    greet(partner)
    pl.when(has_left)(lambda: greet(me - 2))
    pl.when(has_right)(lambda: greet(me + 2))

    sources = (
        feat_hbm, corners_hbm, bilinear_hbm, attention_hbm, w_value_hbm, b_value_hbm,
        w_out_hbm, b_out_hbm, gain1_hbm, bias1_hbm, w_in_hbm, b_in_hbm, w_ff_hbm, b_ff_hbm,
        gain2_hbm, bias2_hbm,
    )
    targets = (
        gathered.at[me], corners, bilinear, attention, w_value, b_value,
        w_out, b_out, gain1, bias1, w_in, b_in, w_ff, b_ff, gain2, bias2,
    )
    loads = [
        pltpu.make_async_copy(source, target, load_sem.at[number])
        for number, (source, target) in enumerate(zip(sources, targets))
    ]
    for load in loads:
        load.start()

    def copy_of(block, cut, target, lane):
        begin, count = cuts[cut]
        part = gathered.at[block, pl.ds(begin, count)]
        return pltpu.make_async_remote_copy(
            src_ref=part,
            dst_ref=part,
            send_sem=send_sem.at[lane, block, cut],
            recv_sem=recv_sem.at[block, cut],
            device_id={"band": target},
            device_id_type=MESH,
        )

    both = jnp.minimum(mine_z, line - 1 - mine_z)
    more_right = mine_z * 2 < line

    def arrival(number):
        paired = number <= 2 * both
        from_left = jnp.where(paired, number % 2 == 1, jnp.logical_not(more_right))
        distance = jnp.where(paired, (number + 1) // 2, number - both)
        return from_left, mine_z + jnp.where(from_left, -distance, distance)

    def onward(number):
        from_left, place = arrival(number)
        target = jnp.where(from_left, me + 2, me - 2)
        exists = jnp.where(from_left, has_right, has_left)
        return place * 2 + mine_y, place * 2 + 1 - mine_y, target, exists

    loads[0].wait()
    pl.semaphore_wait(
        barrier, 1 + has_left.astype(jnp.int32) + has_right.astype(jnp.int32)
    )
    for cut in range(len(cuts)):
        pl.when(has_left)(copy_of(me, cut, me - 2, 0).start)
        pl.when(has_right)(copy_of(me, cut, me + 2, 1).start)
        copy_of(me, cut, partner, 2).start()

    def forward(number, cut):
        block, _, target, exists = onward(number)
        copy_of(block, cut, partner, 2).wait_recv()
        pl.when(exists)(copy_of(block, cut, target, 0).start)
        copy_of(block, cut, partner, 2).start()

    for load in loads[1:6]:
        load.wait()
    w_value_t[...] = jnp.transpose(w_value[...].astype(F32)).astype(BF16)
    shift_t[...] = jnp.transpose(jnp.broadcast_to(b_value[...], (LANES, model)))

    def turned(block):
        tail = jnp.zeros((padded - tokens, block.shape[1]), F32)
        table = jnp.transpose(jnp.concatenate([block, tail], axis=0))
        return [table[:, half * LANES : (half + 1) * LANES] for half in range(halves)]

    for half, table in enumerate(turned(corners[...].astype(F32))):
        turned_t[half] = table
    level_of = lax.broadcasted_iota(jnp.int32, (points, LANES), 0) // POINTS % LEVELS
    width_of = jnp.where(level_of == 0, float(widths[0]), float(widths[1]))
    inverse = jnp.where(level_of == 0, 1.0 / widths[0], 1.0 / widths[1])
    for half in range(halves):
        place = turned_t[half, pl.ds(0, points, stride=4), :]
        place_t[half] = place
        row = jnp.floor((place + 0.5) * inverse)
        row_t[half] = row
        column_t[half] = place - row * width_of
        row = jnp.floor((place + 1.5) * inverse)
        row_next_t[half] = row
        column_next_t[half] = place + 1.0 - row * width_of
    for half, table in enumerate(turned(bilinear[...])):
        turned_t[half] = table
    for half, share in enumerate(turned(attention[...])):
        for corner in range(4):
            product = share * turned_t[half, pl.ds(corner, points, stride=4), :]
            weight_t[corner, half] = product.astype(BF16).astype(F32)
    samp_t[...] = jnp.zeros(samp_t.shape, F32)

    iota = lax.broadcasted_iota(jnp.int32, (UNIT, LANES), 0).astype(F32)
    zero = jnp.zeros((UNIT, LANES), BF16)

    def spread(table, *at):
        *lead, point = at
        return jnp.broadcast_to(table[(*lead, pl.ds(point, 1), slice(None))], (UNIT, LANES))

    def build(piece, carry):
        head, half = piece // halves, piece % halves
        for level in (0, 1):
            width, count = widths[level], rows[level]
            total = count * bands // width
            base = (head * LEVELS + level) * POINTS
            spans = min(width, 4 * UNIT)
            own_row = [spread(row_t, half, base + which).astype(BF16) for which in range(POINTS)]
            own_column = [
                spread(column_t, half, base + which).astype(BF16) for which in range(POINTS)
            ]
            next_row = [
                spread(row_next_t, half, base + which).astype(BF16) for which in range(POINTS)
            ]
            next_column = [
                spread(column_next_t, half, base + which).astype(BF16) for which in range(POINTS)
            ]
            weight = [
                [spread(weight_t, corner, half, base + which).astype(BF16) for corner in range(4)]
                for which in range(POINTS)
            ]
            for first in range(0, width, spans):
                top, bottom = [], []
                for unit in range(first, first + spans, UNIT):
                    at = (iota + float(unit)).astype(BF16)
                    for which in range(POINTS):
                        left = at == own_column[which]
                        right = at == next_column[which]
                        w = weight[which]
                        top.append(jnp.where(left, w[0], jnp.where(right, w[1], zero)))
                        bottom.append(jnp.where(left, w[2], jnp.where(right, w[3], zero)))
                before = None
                for row in range(total):
                    now = [value == float(row) for value in own_row]
                    turn = [value == float(row) for value in next_row] if first == 0 else now
                    for number in range(spans // UNIT):
                        masks = turn if number == 0 else now
                        earlier = None if before is None else before[0 if number == 0 else 1]
                        entry = None
                        for which in range(POINTS):
                            index = number * POINTS + which
                            under = (
                                zero
                                if earlier is None
                                else jnp.where(earlier[which], bottom[index], zero)
                            )
                            term = jnp.where(masks[which], top[index], under)
                            entry = term if entry is None else entry + term
                        place = row * width + first + number * UNIT
                        block, inside = place // count, starts[level] + place % count
                        matrix[block, head, half, inside : inside + UNIT, :] = entry
                    before = (turn, now)
        exact = max(rows[2], rows[3]) * bands <= 256
        kind = BF16 if exact else F32
        begin = padded - UNIT
        row_at = iota + float(begin)
        third = row_at < float(starts[3])
        valid = row_at < float(starts[3] + rows[3])
        unit_zero = jnp.zeros((UNIT, LANES), kind)

        def mixed(table, *at):
            pair = [
                spread(table, *at, (head * LEVELS + level) * POINTS + which) for level in (2, 3)
            ]
            return jnp.where(third, pair[0], pair[1]).astype(kind)

        coarse = []
        for which in range(POINTS):
            coarse.append(
                (
                    mixed(place_t, half),
                    [mixed(weight_t, corner, half) for corner in range(4)],
                )
            )
        for block in range(bands):
            position = jnp.where(
                third,
                row_at + float(block * rows[2] - starts[2]),
                jnp.where(valid, row_at + float(block * rows[3] - starts[3]), -1000.0),
            )
            under = position - jnp.where(third, float(widths[2]), float(widths[3]))
            spots = [
                spot.astype(kind) for spot in (position, position - 1.0, under, under - 1.0)
            ]
            entry = None
            for place, weights in coarse:
                term = unit_zero
                for spot, weight in zip(spots, weights):
                    term = jnp.where(spot == place, weight, term)
                entry = term if entry is None else entry + term
            matrix[block, head, half, begin:padded, :] = entry.astype(BF16)
        return carry

    lane = lax.broadcasted_iota(jnp.int32, (model, LANES), 1)

    def consume(block):
        value_t = lax.dot_general(
            w_value_t[...], gathered[block], (((1,), (1,)), ((), ())), preferred_element_type=F32
        )
        pieces = []
        for half in range(halves):
            stop = min(tokens, (half + 1) * LANES)
            part = value_t[:, half * LANES : stop]
            count = stop - half * LANES
            if count < LANES:
                part = jnp.concatenate(
                    [part, jnp.zeros((model, LANES - count), F32)], axis=1
                )
            part = part + shift_t[...]
            if count < LANES:
                part = jnp.where(lane < count, part, 0.0)
            pieces.append(part.astype(BF16))
        value = jnp.concatenate(pieces, axis=1)
        for head in range(HEADS):
            into = slice(head * head_dim, (head + 1) * head_dim)
            lookup = jnp.concatenate([matrix[block, head, half] for half in range(halves)], axis=1)
            samp_t[into, :] += jnp.dot(value[into, :], lookup, preferred_element_type=F32)

    stages = [(number, cut) for number in range(1, line) for cut in range(len(cuts))]
    everything = HEADS * halves
    done = 0
    ready = []
    for index, (number, cut) in enumerate(stages):
        upto = everything if index >= len(BUILT) else min(everything, BUILT[index])
        if upto > done:
            lax.fori_loop(done, upto, build, 0)
            done = upto
            if done == everything:
                consume(me)
        elif ready:
            consume(ready.pop(0))
        forward(number, cut)
        if cut == len(cuts) - 1:
            ready.append(onward(number)[0])
    if done < everything:
        lax.fori_loop(done, everything, build, 0)
        consume(me)
    across = [partner] + [onward(number)[1] for number in range(1, line)]

    def consume_across(block):
        for cut in range(len(cuts)):
            copy_of(block, cut, partner, 2).wait_recv()
        consume(block)

    for block in across[:-1]:
        consume_across(block)
        if ready:
            consume(ready.pop(0))
    for block in ready:
        consume(block)
    consume_across(across[-1])

    for load in loads[6:]:
        load.wait()
    sampled = jnp.transpose(samp_t[...])[0:tokens, :].astype(BF16)
    attended = jnp.dot(sampled, w_out[...], preferred_element_type=F32) + b_out[...]
    middle = norm(gathered[me].astype(F32) + attended, gain1[...], bias1[...]).astype(BF16)
    hidden = jnp.maximum(
        jnp.dot(middle, w_in[...], preferred_element_type=F32) + b_in[...], 0.0
    ).astype(BF16)
    result = (
        middle.astype(F32)
        + jnp.dot(hidden, w_ff[...], preferred_element_type=F32)
        + b_ff[...]
    )
    out[...] = norm(result, gain2[...], bias2[...]).astype(BF16)

    for cut in range(len(cuts)):
        pl.when(has_left)(copy_of(me, cut, me - 2, 0).wait_send)
        pl.when(has_right)(copy_of(me, cut, me + 2, 1).wait_send)
        copy_of(me, cut, partner, 2).wait_send()
        for number in range(1, line):
            block, _, target, exists = onward(number)
            pl.when(exists)(copy_of(block, cut, target, 0).wait_send)
            copy_of(block, cut, partner, 2).wait_send()


def body(bands, *args):
    tokens, model = args[0].shape
    padded = -(-tokens // LANES) * LANES
    halves = padded // LANES
    samples = args[1].shape[1]
    points = samples // 4
    operands = [
        argument.reshape(1, -1) if argument.ndim == 1 else argument for argument in args
    ]
    cuts = -(-tokens // CHUNK)
    table = pltpu.VMEM((halves, points, LANES), F32)
    scratch = [
        pltpu.VMEM((bands, tokens, model), BF16),
        *(pltpu.VMEM(operand.shape, operand.dtype) for operand in operands[1:]),
        pltpu.VMEM(args[4].shape, BF16),
        pltpu.VMEM((model, LANES), F32),
        pltpu.VMEM((halves, samples, LANES), F32),
        table,
        table,
        table,
        table,
        table,
        pltpu.VMEM((4, halves, points, LANES), F32),
        pltpu.VMEM((bands, HEADS, halves, padded, LANES), BF16),
        pltpu.VMEM((model, padded), F32),
        pltpu.SemaphoreType.DMA((3, bands, cuts)),
        pltpu.SemaphoreType.DMA((bands, cuts)),
        pltpu.SemaphoreType.DMA((len(operands),)),
    ]
    return pl.pallas_call(
        functools.partial(kernel, bands),
        out_shape=jax.ShapeDtypeStruct((tokens, model), BF16),
        in_specs=[pl.BlockSpec(memory_space=pl.ANY)] * len(operands),
        out_specs=pl.BlockSpec(memory_space=pltpu.VMEM),
        scratch_shapes=scratch,
        compiler_params=pltpu.CompilerParams(
            collective_id=0, has_side_effects=True, vmem_limit_bytes=60 * 1024 * 1024
        ),
        name="layer",
    )(*operands)


def solution(mesh):
    split = P(("dp", "band"), None)
    in_specs = (split,) * 4 + (P(),) * 12
    return jax.shard_map(
        functools.partial(body, mesh.shape["band"]),
        mesh=mesh,
        in_specs=in_specs,
        out_specs=split,
        check_vma=False,
    )
```

```python
import functools

import jax
import jax.numpy as jnp
from jax import lax
from jax.experimental import pallas as pl
from jax.experimental.pallas import tpu as pltpu
from jax.sharding import PartitionSpec as P

HEADS = 8
LEVELS = 4
POINTS = 4
ROWS_DEV = 192
MAP_W = 128
LANES = 128
UNIT = 16
CHUNK = 64
AHEAD = 6

F32 = jnp.float32
BF16 = jnp.bfloat16
MESH = pl.DeviceIdType.MESH


def norm(inputs, gain, shift):
    average = jnp.mean(inputs, axis=-1, keepdims=True)
    centred = inputs - average
    variance = jnp.mean(centred * centred, axis=-1, keepdims=True)
    return centred * lax.rsqrt(variance + 1e-05) * gain + shift


def kernel(
    bands,
    feat_hbm,
    corners_hbm,
    bilinear_hbm,
    attention_hbm,
    w_value_hbm,
    b_value_hbm,
    w_out_hbm,
    b_out_hbm,
    gain1_hbm,
    bias1_hbm,
    w_in_hbm,
    b_in_hbm,
    w_ff_hbm,
    b_ff_hbm,
    gain2_hbm,
    bias2_hbm,
    out,
    gathered,
    corners,
    bilinear,
    attention,
    w_value,
    b_value,
    w_out,
    b_out,
    gain1,
    bias1,
    w_in,
    b_in,
    w_ff,
    b_ff,
    gain2,
    bias2,
    w_value_t,
    shift_t,
    turned_t,
    row_t,
    column_t,
    row_next_t,
    column_next_t,
    place_t,
    weight_t,
    matrix,
    samp_t,
    line_sem,
    across_sem,
    recv_sem,
    cross_sem,
    load_sem,
):
    rows = [ROWS_DEV // 4**level for level in range(LEVELS)]
    starts = [sum(rows[:level]) for level in range(LEVELS)]
    widths = [MAP_W // 2**level for level in range(LEVELS)]
    tokens, model = feat_hbm.shape
    head_dim = model // HEADS
    padded = matrix.shape[3]
    halves = matrix.shape[2]
    points = HEADS * LEVELS * POINTS
    me = lax.axis_index("band")

    line = bands // 2
    mine_z, mine_y = me // 2, lax.rem(me, 2)
    partner = mine_z * 2 + 1 - mine_y
    cuts = [(begin, min(begin + CHUNK, tokens) - begin) for begin in range(0, tokens, CHUNK)]

    barrier = pltpu.get_barrier_semaphore()

    def greet(target):
        pl.semaphore_signal(barrier, inc=1, device_id={"band": target}, device_id_type=MESH)

    at_start, at_stop = mine_z == 0, mine_z == line - 1
    direct = [(mine_z > 0, me - 2), (mine_z < line - 1, me + 2)]
    greeted = [*direct]
    if line > 2:
        direct.append((at_stop, mine_y))
        greeted.append((at_start, (line - 1) * 2 + mine_y))
    greet(partner)
    for exists, target in greeted:
        pl.when(exists)(functools.partial(greet, target))

    sources = (
        feat_hbm, corners_hbm, bilinear_hbm, attention_hbm, w_value_hbm, b_value_hbm,
        w_out_hbm, b_out_hbm, gain1_hbm, bias1_hbm, w_in_hbm, b_in_hbm, w_ff_hbm, b_ff_hbm,
        gain2_hbm, bias2_hbm,
    )
    targets = (
        gathered.at[me], corners, bilinear, attention, w_value, b_value,
        w_out, b_out, gain1, bias1, w_in, b_in, w_ff, b_ff, gain2, bias2,
    )
    loads = [
        pltpu.make_async_copy(source, target, load_sem.at[number])
        for number, (source, target) in enumerate(zip(sources, targets))
    ]
    for load in loads:
        load.start()

    def move(part, target, send, receive):
        return pltpu.make_async_remote_copy(
            src_ref=part,
            dst_ref=part,
            send_sem=send,
            recv_sem=receive,
            device_id={"band": target},
            device_id_type=MESH,
        )

    def along_line(block, cut, target, way):
        part = gathered.at[block, pl.ds(*cuts[cut])] if cut is not None else gathered.at[block]
        receive = recv_sem.at[block // 2, cut or 0]
        return move(part, target, line_sem.at[way], receive)

    def across(block, cut, way):
        part = gathered.at[block, pl.ds(*cuts[cut])] if cut is not None else gathered.at[block]
        return move(part, partner, across_sem.at[way], cross_sem.at[block // 2])

    both = jnp.minimum(mine_z, line - 1 - mine_z)
    more_right = mine_z * 2 < line

    def arrival(number):
        paired = number <= 2 * both
        from_left = jnp.where(paired, number % 2 == 0, jnp.logical_not(more_right))
        distance = jnp.where(paired, (number + 1) // 2, number - both)
        skipped = line - 1 if number == 2 else max(number - 1, 1)
        distance = jnp.where(at_start, skipped, distance)
        place = mine_z + jnp.where(from_left, -distance, distance)
        onto = jnp.where(from_left, mine_z + 1, mine_z - 1)
        exists = jnp.logical_and(onto >= 0, onto < line)
        if line > 2:
            exists = jnp.logical_and(exists, onto - place != 1 - line)
        return place, exists, onto * 2 + mine_y

    arrivals = [arrival(number) for number in range(1, line)]
    near = [place * 2 + mine_y for place, _, _ in arrivals]
    far = [place * 2 + 1 - mine_y for place, _, _ in arrivals]

    loads[0].wait()
    pl.semaphore_wait(barrier, 1 + sum(exists.astype(jnp.int32) for exists, _ in direct))
    for cut in range(len(cuts)):
        for way in reversed(range(len(direct))):
            exists, target = direct[way]
            pl.when(exists)(along_line(me, cut, target, way).start)
        across(me, cut, 0).start()

    def forward(number, cut):
        block = near[number]
        _, exists, target = arrivals[number]
        copy = along_line(block, cut, target, len(direct) + number)
        copy.wait_recv()
        pl.when(exists)(copy.start)
        across(block, cut, 1 + number).start()

    for load in loads[1:6]:
        load.wait()
    w_value_t[...] = jnp.transpose(w_value[...].astype(F32)).astype(BF16)
    shift_t[...] = jnp.transpose(jnp.broadcast_to(b_value[...], (LANES, model)))

    def turned(block):
        tail = jnp.zeros((padded - tokens, block.shape[1]), F32)
        table = jnp.transpose(jnp.concatenate([block, tail], axis=0))
        return [table[:, half * LANES : (half + 1) * LANES] for half in range(halves)]

    for half, table in enumerate(turned(corners[...].astype(F32))):
        turned_t[half] = table
    level_of = lax.broadcasted_iota(jnp.int32, (points, LANES), 0) // POINTS % LEVELS
    width_of = jnp.where(level_of == 0, float(widths[0]), float(widths[1]))
    inverse = jnp.where(level_of == 0, 1.0 / widths[0], 1.0 / widths[1])
    for half in range(halves):
        place = turned_t[half, pl.ds(0, points, stride=4), :]
        place_t[half] = place
        row = jnp.floor((place + 0.5) * inverse)
        row_t[half] = row
        column_t[half] = place - row * width_of
        row = jnp.floor((place + 1.5) * inverse)
        row_next_t[half] = row
        column_next_t[half] = place + 1.0 - row * width_of
    for half, table in enumerate(turned(bilinear[...])):
        turned_t[half] = table
    for half, share in enumerate(turned(attention[...])):
        for corner in range(4):
            product = share * turned_t[half, pl.ds(corner, points, stride=4), :]
            weight_t[corner, half] = product.astype(BF16).astype(F32)
    samp_t[...] = jnp.zeros(samp_t.shape, F32)

    iota = lax.broadcasted_iota(jnp.int32, (UNIT, LANES), 0).astype(F32)
    zero = jnp.zeros((UNIT, LANES), BF16)

    def spread(table, *at):
        *lead, point = at
        return jnp.broadcast_to(table[(*lead, pl.ds(point, 1), slice(None))], (UNIT, LANES))

    def build(piece, carry):
        head, half = piece // halves, piece % halves
        for level in (0, 1):
            width, count = widths[level], rows[level]
            total = count * bands // width
            base = (head * LEVELS + level) * POINTS
            spans = min(width, 4 * UNIT)
            own_row = [spread(row_t, half, base + which).astype(BF16) for which in range(POINTS)]
            own_column = [
                spread(column_t, half, base + which).astype(BF16) for which in range(POINTS)
            ]
            next_row = [
                spread(row_next_t, half, base + which).astype(BF16) for which in range(POINTS)
            ]
            next_column = [
                spread(column_next_t, half, base + which).astype(BF16) for which in range(POINTS)
            ]
            weight = [
                [spread(weight_t, corner, half, base + which).astype(BF16) for corner in range(4)]
                for which in range(POINTS)
            ]
            for first in range(0, width, spans):
                top, bottom = [], []
                for unit in range(first, first + spans, UNIT):
                    at = (iota + float(unit)).astype(BF16)
                    for which in range(POINTS):
                        left = at == own_column[which]
                        right = at == next_column[which]
                        w = weight[which]
                        top.append(jnp.where(left, w[0], jnp.where(right, w[1], zero)))
                        bottom.append(jnp.where(left, w[2], jnp.where(right, w[3], zero)))
                before = None
                for row in range(total):
                    now = [value == float(row) for value in own_row]
                    turn = [value == float(row) for value in next_row] if first == 0 else now
                    for number in range(spans // UNIT):
                        masks = turn if number == 0 else now
                        earlier = None if before is None else before[0 if number == 0 else 1]
                        entry = None
                        for which in range(POINTS):
                            index = number * POINTS + which
                            under = (
                                zero
                                if earlier is None
                                else jnp.where(earlier[which], bottom[index], zero)
                            )
                            term = jnp.where(masks[which], top[index], under)
                            entry = term if entry is None else entry + term
                        place = row * width + first + number * UNIT
                        block, inside = place // count, starts[level] + place % count
                        matrix[block, head, half, inside : inside + UNIT, :] = entry
                    before = (turn, now)
        exact = max(rows[2], rows[3]) * bands <= 256
        kind = BF16 if exact else F32
        begin = padded - UNIT
        row_at = iota + float(begin)
        third = row_at < float(starts[3])
        valid = row_at < float(starts[3] + rows[3])
        unit_zero = jnp.zeros((UNIT, LANES), kind)

        def mixed(table, *at):
            pair = [
                spread(table, *at, (head * LEVELS + level) * POINTS + which) for level in (2, 3)
            ]
            return jnp.where(third, pair[0], pair[1]).astype(kind)

        coarse = []
        for which in range(POINTS):
            coarse.append(
                (
                    mixed(place_t, half),
                    [mixed(weight_t, corner, half) for corner in range(4)],
                )
            )
        for block in range(bands):
            position = jnp.where(
                third,
                row_at + float(block * rows[2] - starts[2]),
                jnp.where(valid, row_at + float(block * rows[3] - starts[3]), -1000.0),
            )
            under = position - jnp.where(third, float(widths[2]), float(widths[3]))
            spots = [
                spot.astype(kind) for spot in (position, position - 1.0, under, under - 1.0)
            ]
            entry = None
            for place, weights in coarse:
                term = unit_zero
                for spot, weight in zip(spots, weights):
                    term = jnp.where(spot == place, weight, term)
                entry = term if entry is None else entry + term
            matrix[block, head, half, begin:padded, :] = entry.astype(BF16)
        return carry

    lane = lax.broadcasted_iota(jnp.int32, (model, LANES), 1)

    def consume(block):
        value_t = lax.dot_general(
            w_value_t[...], gathered[block], (((1,), (1,)), ((), ())), preferred_element_type=F32
        )
        pieces = []
        for half in range(halves):
            stop = min(tokens, (half + 1) * LANES)
            part = value_t[:, half * LANES : stop]
            count = stop - half * LANES
            if count < LANES:
                part = jnp.concatenate(
                    [part, jnp.zeros((model, LANES - count), F32)], axis=1
                )
            part = part + shift_t[...]
            if count < LANES:
                part = jnp.where(lane < count, part, 0.0)
            pieces.append(part.astype(BF16))
        value = jnp.concatenate(pieces, axis=1)
        for head in range(HEADS):
            into = slice(head * head_dim, (head + 1) * head_dim)
            lookup = jnp.concatenate([matrix[block, head, half] for half in range(halves)], axis=1)
            samp_t[into, :] += jnp.dot(value[into, :], lookup, preferred_element_type=F32)

    def consume_across(block):
        across(block, None, 0).wait_recv()
        consume(block)

    everything = HEADS * halves
    done = 0
    for index, (cut, number) in enumerate(
        [(cut, number) for cut in range(len(cuts)) for number in range(min(2, line - 1))]
        + [(cut, number) for number in range(2, line - 1) for cut in range(len(cuts))]
    ):
        upto = min(everything, AHEAD + index)
        if upto > done:
            lax.fori_loop(done, upto, build, 0)
            done = upto
        forward(number, cut)
    if done < everything:
        lax.fori_loop(done, everything, build, 0)
    consume(me)
    consume_across(partner)
    for number in range(line - 1):
        consume(near[number])
        if number:
            consume_across(far[number - 1])
    consume_across(far[line - 2])

    for load in loads[6:]:
        load.wait()
    sampled = jnp.transpose(samp_t[...])[0:tokens, :].astype(BF16)
    attended = jnp.dot(sampled, w_out[...], preferred_element_type=F32) + b_out[...]
    middle = norm(gathered[me].astype(F32) + attended, gain1[...], bias1[...]).astype(BF16)
    hidden = jnp.maximum(
        jnp.dot(middle, w_in[...], preferred_element_type=F32) + b_in[...], 0.0
    ).astype(BF16)
    result = (
        middle.astype(F32)
        + jnp.dot(hidden, w_ff[...], preferred_element_type=F32)
        + b_ff[...]
    )
    out[...] = norm(result, gain2[...], bias2[...]).astype(BF16)

    for way, (exists, target) in enumerate(direct):
        pl.when(exists)(along_line(me, None, target, way).wait_send)
    across(me, None, 0).wait_send()
    for number, (_, exists, target) in enumerate(arrivals):
        pl.when(exists)(
            along_line(near[number], None, target, len(direct) + number).wait_send
        )
        across(near[number], None, 1 + number).wait_send()


def body(bands, *args):
    tokens, model = args[0].shape
    padded = -(-tokens // LANES) * LANES
    halves = padded // LANES
    samples = args[1].shape[1]
    points = samples // 4
    operands = [
        argument.reshape(1, -1) if argument.ndim == 1 else argument for argument in args
    ]
    cuts = -(-tokens // CHUNK)
    table = pltpu.VMEM((halves, points, LANES), F32)
    scratch = [
        pltpu.VMEM((bands, tokens, model), BF16),
        *(pltpu.VMEM(operand.shape, operand.dtype) for operand in operands[1:]),
        pltpu.VMEM(args[4].shape, BF16),
        pltpu.VMEM((model, LANES), F32),
        pltpu.VMEM((halves, samples, LANES), F32),
        table,
        table,
        table,
        table,
        table,
        pltpu.VMEM((4, halves, points, LANES), F32),
        pltpu.VMEM((bands, HEADS, halves, padded, LANES), BF16),
        pltpu.VMEM((model, padded), F32),
        pltpu.SemaphoreType.DMA((2 + bands // 2,)),
        pltpu.SemaphoreType.DMA((bands // 2,)),
        pltpu.SemaphoreType.DMA((bands // 2, cuts)),
        pltpu.SemaphoreType.DMA((bands // 2,)),
        pltpu.SemaphoreType.DMA((len(operands),)),
    ]
    held = bands * HEADS * padded * padded * 2 + bands * tokens * model * 2
    limit = held + 16 * 1024 * 1024
    return pl.pallas_call(
        functools.partial(kernel, bands),
        out_shape=jax.ShapeDtypeStruct((tokens, model), BF16),
        in_specs=[pl.BlockSpec(memory_space=pl.ANY)] * len(operands),
        out_specs=pl.BlockSpec(memory_space=pltpu.VMEM),
        scratch_shapes=scratch,
        compiler_params=pltpu.CompilerParams(
            collective_id=0, has_side_effects=True, vmem_limit_bytes=limit
        ),
        name="layer",
    )(*(pltpu.with_memory_space_constraint(operand, pltpu.HBM) for operand in operands))


def solution(mesh):
    split = P(("dp", "band"), None)
    in_specs = (split,) * 4 + (P(),) * 12
    return jax.shard_map(
        functools.partial(body, mesh.shape["band"]),
        mesh=mesh,
        in_specs=in_specs,
        out_specs=split,
        check_vma=False,
    )
```

```python
import functools

import jax
import jax.numpy as jnp
from jax import lax
from jax.experimental import pallas as pl
from jax.experimental.pallas import tpu as pltpu
from jax.sharding import PartitionSpec as P

HEADS = 8
LEVELS = 4
POINTS = 4
ROWS_DEV = 192
MAP_W = 128
LANES = 128
UNIT = 16
CHUNK = 64
SLANTED = 3
AHEAD = 6

F32 = jnp.float32
BF16 = jnp.bfloat16
MESH = pl.DeviceIdType.MESH


def norm(inputs, gain, shift):
    average = jnp.mean(inputs, axis=-1, keepdims=True)
    centred = inputs - average
    variance = jnp.mean(centred * centred, axis=-1, keepdims=True)
    return centred * lax.rsqrt(variance + 1e-05) * gain + shift


def kernel(
    bands,
    feat_hbm,
    corners_hbm,
    bilinear_hbm,
    attention_hbm,
    w_value_hbm,
    b_value_hbm,
    w_out_hbm,
    b_out_hbm,
    gain1_hbm,
    bias1_hbm,
    w_in_hbm,
    b_in_hbm,
    w_ff_hbm,
    b_ff_hbm,
    gain2_hbm,
    bias2_hbm,
    out,
    gathered,
    corners,
    bilinear,
    attention,
    w_value,
    b_value,
    w_out,
    b_out,
    gain1,
    bias1,
    w_in,
    b_in,
    w_ff,
    b_ff,
    gain2,
    bias2,
    w_value_t,
    shift_t,
    turned_t,
    row_t,
    column_t,
    row_next_t,
    column_next_t,
    place_t,
    weight_t,
    matrix,
    samp_t,
    line_sem,
    across_sem,
    recv_sem,
    cross_sem,
    load_sem,
):
    rows = [ROWS_DEV // 4**level for level in range(LEVELS)]
    starts = [sum(rows[:level]) for level in range(LEVELS)]
    widths = [MAP_W // 2**level for level in range(LEVELS)]
    tokens, model = feat_hbm.shape
    head_dim = model // HEADS
    padded = matrix.shape[3]
    halves = matrix.shape[2]
    points = HEADS * LEVELS * POINTS
    me = lax.axis_index("band")

    line = bands // 2
    mine_z, mine_y = me // 2, lax.rem(me, 2)
    partner = mine_z * 2 + 1 - mine_y
    cuts = [(begin, min(begin + CHUNK, tokens) - begin) for begin in range(0, tokens, CHUNK)]

    barrier = pltpu.get_barrier_semaphore()

    def greet(target):
        pl.semaphore_signal(barrier, inc=1, device_id={"band": target}, device_id_type=MESH)

    at_start, at_stop = mine_z == 0, mine_z == line - 1
    direct = [(mine_z > 0, me - 2), (mine_z < line - 1, me + 2)]
    greeted = [*direct]
    if line > 2:
        direct.append((at_stop, mine_y))
        greeted.append((at_start, (line - 1) * 2 + mine_y))
    slanted = [(at_stop, 1 - mine_y)] if line > 2 else []
    greet(partner)
    if line > 2:
        greeted.append((at_start, line * 2 - 1 - mine_y))
    for exists, target in greeted:
        pl.when(exists)(functools.partial(greet, target))

    sources = (
        feat_hbm, corners_hbm, bilinear_hbm, attention_hbm, w_value_hbm, b_value_hbm,
        w_out_hbm, b_out_hbm, gain1_hbm, bias1_hbm, w_in_hbm, b_in_hbm, w_ff_hbm, b_ff_hbm,
        gain2_hbm, bias2_hbm,
    )
    targets = (
        gathered.at[me], corners, bilinear, attention, w_value, b_value,
        w_out, b_out, gain1, bias1, w_in, b_in, w_ff, b_ff, gain2, bias2,
    )
    loads = [
        pltpu.make_async_copy(source, target, load_sem.at[number])
        for number, (source, target) in enumerate(zip(sources, targets))
    ]
    for load in loads:
        load.start()

    def move(part, target, send, receive):
        return pltpu.make_async_remote_copy(
            src_ref=part,
            dst_ref=part,
            send_sem=send,
            recv_sem=receive,
            device_id={"band": target},
            device_id_type=MESH,
        )

    def along_line(block, cut, target, way):
        part = gathered.at[block, pl.ds(*cuts[cut])] if cut is not None else gathered.at[block]
        receive = recv_sem.at[block // 2, cut or 0]
        return move(part, target, line_sem.at[way], receive)

    def across(block, cut, way):
        part = gathered.at[block, pl.ds(*cuts[cut])] if cut is not None else gathered.at[block]
        return move(part, partner, across_sem.at[way], cross_sem.at[block // 2])

    later = pl.ds(cuts[SLANTED][0], tokens - cuts[SLANTED][0])
    sooner = pl.ds(0, cuts[SLANTED][0])

    def slant(cut, target):
        part = gathered.at[me, pl.ds(*cuts[cut]) if cut is not None else later]
        return move(part, target, line_sem.at[2 * line], cross_sem.at[mine_z])

    both = jnp.minimum(mine_z, line - 1 - mine_z)
    more_right = mine_z * 2 < line

    def arrival(number):
        paired = number <= 2 * both
        from_left = jnp.where(paired, number % 2 == 0, jnp.logical_not(more_right))
        distance = jnp.where(paired, (number + 1) // 2, number - both)
        skipped = line - 1 if number == 2 else max(number - 1, 1)
        distance = jnp.where(at_start, skipped, distance)
        place = mine_z + jnp.where(from_left, -distance, distance)
        onto = jnp.where(from_left, mine_z + 1, mine_z - 1)
        exists = jnp.logical_and(onto >= 0, onto < line)
        if line > 2:
            exists = jnp.logical_and(exists, onto - place != 1 - line)
        return place, exists, onto * 2 + mine_y

    arrivals = [arrival(number) for number in range(1, line)]
    near = [place * 2 + mine_y for place, _, _ in arrivals]
    far = [place * 2 + 1 - mine_y for place, _, _ in arrivals]

    loads[0].wait()
    pl.semaphore_wait(barrier, 1 + sum(exists.astype(jnp.int32) for exists, _ in [*direct, *slanted]))
    for cut in range(len(cuts)):
        for way in range(2):
            exists, target = direct[way]
            pl.when(exists)(along_line(me, cut, target, way).start)
        across(me, cut, 0).start()
    for cut in range(len(cuts)):
        for way in range(2, len(direct)):
            exists, target = direct[way]
            pl.when(exists)(along_line(me, cut, target, way).start)
        if cut >= SLANTED:
            for exists, target in slanted:
                pl.when(exists)(slant(cut, target).start)

    def forward(number, cut):
        block = near[number]
        _, exists, target = arrivals[number]
        copy = along_line(block, cut, target, len(direct) + number)
        copy.wait_recv()
        pl.when(exists)(copy.start)
        if line > 2 and cut >= SLANTED:
            spared = jnp.logical_and(at_start, block // 2 == line - 1)
            pl.when(jnp.logical_not(spared))(across(block, cut, 1 + number).start)
        else:
            across(block, cut, 1 + number).start()

    for load in loads[1:6]:
        load.wait()
    w_value_t[...] = jnp.transpose(w_value[...].astype(F32)).astype(BF16)
    shift_t[...] = jnp.transpose(jnp.broadcast_to(b_value[...], (LANES, model)))

    def turned(block):
        tail = jnp.zeros((padded - tokens, block.shape[1]), F32)
        table = jnp.transpose(jnp.concatenate([block, tail], axis=0))
        return [table[:, half * LANES : (half + 1) * LANES] for half in range(halves)]

    for half, table in enumerate(turned(corners[...].astype(F32))):
        turned_t[half] = table
    level_of = lax.broadcasted_iota(jnp.int32, (points, LANES), 0) // POINTS % LEVELS
    width_of = jnp.where(level_of == 0, float(widths[0]), float(widths[1]))
    inverse = jnp.where(level_of == 0, 1.0 / widths[0], 1.0 / widths[1])
    for half in range(halves):
        place = turned_t[half, pl.ds(0, points, stride=4), :]
        place_t[half] = place
        row = jnp.floor((place + 0.5) * inverse)
        row_t[half] = row
        column_t[half] = place - row * width_of
        row = jnp.floor((place + 1.5) * inverse)
        row_next_t[half] = row
        column_next_t[half] = place + 1.0 - row * width_of
    for half, table in enumerate(turned(bilinear[...])):
        turned_t[half] = table
    for half, share in enumerate(turned(attention[...])):
        for corner in range(4):
            product = share * turned_t[half, pl.ds(corner, points, stride=4), :]
            weight_t[corner, half] = product.astype(BF16).astype(F32)
    samp_t[...] = jnp.zeros(samp_t.shape, F32)

    iota = lax.broadcasted_iota(jnp.int32, (UNIT, LANES), 0).astype(F32)
    zero = jnp.zeros((UNIT, LANES), BF16)

    def spread(table, *at):
        *lead, point = at
        return jnp.broadcast_to(table[(*lead, pl.ds(point, 1), slice(None))], (UNIT, LANES))

    def build(piece, carry):
        head, half = piece // halves, piece % halves
        for level in (0, 1):
            width, count = widths[level], rows[level]
            total = count * bands // width
            base = (head * LEVELS + level) * POINTS
            spans = min(width, 4 * UNIT)
            own_row = [spread(row_t, half, base + which).astype(BF16) for which in range(POINTS)]
            own_column = [
                spread(column_t, half, base + which).astype(BF16) for which in range(POINTS)
            ]
            next_row = [
                spread(row_next_t, half, base + which).astype(BF16) for which in range(POINTS)
            ]
            next_column = [
                spread(column_next_t, half, base + which).astype(BF16) for which in range(POINTS)
            ]
            weight = [
                [spread(weight_t, corner, half, base + which).astype(BF16) for corner in range(4)]
                for which in range(POINTS)
            ]
            for first in range(0, width, spans):
                top, bottom = [], []
                for unit in range(first, first + spans, UNIT):
                    at = (iota + float(unit)).astype(BF16)
                    for which in range(POINTS):
                        left = at == own_column[which]
                        right = at == next_column[which]
                        w = weight[which]
                        top.append(jnp.where(left, w[0], jnp.where(right, w[1], zero)))
                        bottom.append(jnp.where(left, w[2], jnp.where(right, w[3], zero)))
                before = None
                for row in range(total):
                    now = [value == float(row) for value in own_row]
                    turn = [value == float(row) for value in next_row] if first == 0 else now
                    for number in range(spans // UNIT):
                        masks = turn if number == 0 else now
                        earlier = None if before is None else before[0 if number == 0 else 1]
                        entry = None
                        for which in range(POINTS):
                            index = number * POINTS + which
                            under = (
                                zero
                                if earlier is None
                                else jnp.where(earlier[which], bottom[index], zero)
                            )
                            term = jnp.where(masks[which], top[index], under)
                            entry = term if entry is None else entry + term
                        place = row * width + first + number * UNIT
                        block, inside = place // count, starts[level] + place % count
                        matrix[block, head, half, inside : inside + UNIT, :] = entry
                    before = (turn, now)
        exact = max(rows[2], rows[3]) * bands <= 256
        kind = BF16 if exact else F32
        begin = padded - UNIT
        row_at = iota + float(begin)
        third = row_at < float(starts[3])
        valid = row_at < float(starts[3] + rows[3])
        unit_zero = jnp.zeros((UNIT, LANES), kind)

        def mixed(table, *at):
            pair = [
                spread(table, *at, (head * LEVELS + level) * POINTS + which) for level in (2, 3)
            ]
            return jnp.where(third, pair[0], pair[1]).astype(kind)

        coarse = []
        for which in range(POINTS):
            coarse.append(
                (
                    mixed(place_t, half),
                    [mixed(weight_t, corner, half) for corner in range(4)],
                )
            )
        for block in range(bands):
            position = jnp.where(
                third,
                row_at + float(block * rows[2] - starts[2]),
                jnp.where(valid, row_at + float(block * rows[3] - starts[3]), -1000.0),
            )
            under = position - jnp.where(third, float(widths[2]), float(widths[3]))
            spots = [
                spot.astype(kind) for spot in (position, position - 1.0, under, under - 1.0)
            ]
            entry = None
            for place, weights in coarse:
                term = unit_zero
                for spot, weight in zip(spots, weights):
                    term = jnp.where(spot == place, weight, term)
                entry = term if entry is None else entry + term
            matrix[block, head, half, begin:padded, :] = entry.astype(BF16)
        return carry

    lane = lax.broadcasted_iota(jnp.int32, (model, LANES), 1)

    def consume(block):
        value_t = lax.dot_general(
            w_value_t[...], gathered[block], (((1,), (1,)), ((), ())), preferred_element_type=F32
        )
        pieces = []
        for half in range(halves):
            stop = min(tokens, (half + 1) * LANES)
            part = value_t[:, half * LANES : stop]
            count = stop - half * LANES
            if count < LANES:
                part = jnp.concatenate(
                    [part, jnp.zeros((model, LANES - count), F32)], axis=1
                )
            part = part + shift_t[...]
            if count < LANES:
                part = jnp.where(lane < count, part, 0.0)
            pieces.append(part.astype(BF16))
        value = jnp.concatenate(pieces, axis=1)
        for head in range(HEADS):
            into = slice(head * head_dim, (head + 1) * head_dim)
            lookup = jnp.concatenate([matrix[block, head, half] for half in range(halves)], axis=1)
            samp_t[into, :] += jnp.dot(value[into, :], lookup, preferred_element_type=F32)

    def consume_across(block):
        across(block, None, 0).wait_recv()
        consume(block)

    everything = HEADS * halves
    done = 0
    for index, (cut, number) in enumerate(
        (cut, number) for number in range(line - 1) for cut in range(len(cuts))
    ):
        upto = min(everything, AHEAD + index)
        if upto > done:
            lax.fori_loop(done, upto, build, 0)
            done = upto
        forward(number, cut)
    if done < everything:
        lax.fori_loop(done, everything, build, 0)
    consume(me)
    consume_across(partner)
    for number in range(line - 1):
        consume(near[number])
        if number:
            consume_across(far[number - 1])
    consume_across(far[line - 2])

    for load in loads[6:]:
        load.wait()
    attended = lax.dot_general(
        samp_t[...].astype(BF16), w_out[...], (((0,), (0,)), ((), ())), preferred_element_type=F32
    )[0:tokens, :] + b_out[...]
    middle = norm(gathered[me].astype(F32) + attended, gain1[...], bias1[...]).astype(BF16)
    hidden = jnp.maximum(
        jnp.dot(middle, w_in[...], preferred_element_type=F32) + b_in[...], 0.0
    ).astype(BF16)
    result = (
        middle.astype(F32)
        + jnp.dot(hidden, w_ff[...], preferred_element_type=F32)
        + b_ff[...]
    )
    out[...] = norm(result, gain2[...], bias2[...]).astype(BF16)

    for way, (exists, target) in enumerate(direct):
        pl.when(exists)(along_line(me, None, target, way).wait_send)
    across(me, None, 0).wait_send()
    for number, (_, exists, target) in enumerate(arrivals):
        pl.when(exists)(
            along_line(near[number], None, target, len(direct) + number).wait_send
        )
        block = near[number]
        if line > 2:
            spared = jnp.logical_and(at_start, block // 2 == line - 1)
            part = gathered.at[block, sooner]
            pl.when(jnp.logical_not(spared))(across(block, None, 1 + number).wait_send)
            pl.when(spared)(
                move(part, partner, across_sem.at[1 + number], cross_sem.at[0]).wait_send
            )
        else:
            across(block, None, 1 + number).wait_send()
    for exists, target in slanted:
        pl.when(exists)(slant(None, target).wait_send)


def body(bands, *args):
    tokens, model = args[0].shape
    padded = -(-tokens // LANES) * LANES
    halves = padded // LANES
    samples = args[1].shape[1]
    points = samples // 4
    operands = [
        argument.reshape(1, -1) if argument.ndim == 1 else argument for argument in args
    ]
    cuts = -(-tokens // CHUNK)
    table = pltpu.VMEM((halves, points, LANES), F32)
    scratch = [
        pltpu.VMEM((bands, tokens, model), BF16),
        *(pltpu.VMEM(operand.shape, operand.dtype) for operand in operands[1:]),
        pltpu.VMEM(args[4].shape, BF16),
        pltpu.VMEM((model, LANES), F32),
        pltpu.VMEM((halves, samples, LANES), F32),
        table,
        table,
        table,
        table,
        table,
        pltpu.VMEM((4, halves, points, LANES), F32),
        pltpu.VMEM((bands, HEADS, halves, padded, LANES), BF16),
        pltpu.VMEM((model, padded), F32),
        pltpu.SemaphoreType.DMA((bands + 1,)),
        pltpu.SemaphoreType.DMA((bands // 2,)),
        pltpu.SemaphoreType.DMA((bands // 2, cuts)),
        pltpu.SemaphoreType.DMA((bands // 2,)),
        pltpu.SemaphoreType.DMA((len(operands),)),
    ]
    held = bands * HEADS * padded * padded * 2 + bands * tokens * model * 2
    limit = held + 16 * 1024 * 1024
    return pl.pallas_call(
        functools.partial(kernel, bands),
        out_shape=jax.ShapeDtypeStruct((tokens, model), BF16),
        in_specs=[pl.BlockSpec(memory_space=pl.ANY)] * len(operands),
        out_specs=pl.BlockSpec(memory_space=pltpu.VMEM),
        scratch_shapes=scratch,
        compiler_params=pltpu.CompilerParams(
            collective_id=0, has_side_effects=True, vmem_limit_bytes=limit
        ),
        name="layer",
    )(*(pltpu.with_memory_space_constraint(operand, pltpu.HBM) for operand in operands))


def solution(mesh):
    split = P(("dp", "band"), None)
    in_specs = (split,) * 4 + (P(),) * 12
    return jax.shard_map(
        functools.partial(body, mesh.shape["band"]),
        mesh=mesh,
        in_specs=in_specs,
        out_specs=split,
        check_vma=False,
    )
```

```python
import functools

import jax
import jax.numpy as jnp
from jax import lax
from jax.experimental import pallas as pl
from jax.experimental.pallas import tpu as pltpu
from jax.sharding import PartitionSpec as P

HEADS = 8
LEVELS = 4
POINTS = 4
ROWS_DEV = 192
MAP_W = 128
LANES = 128
UNIT = 16
CHUNK = 64
LATE = 2
AHEAD = 6

F32 = jnp.float32
BF16 = jnp.bfloat16
MESH = pl.DeviceIdType.MESH


def norm(inputs, gain, shift):
    average = jnp.mean(inputs, axis=-1, keepdims=True)
    centred = inputs - average
    variance = jnp.mean(centred * centred, axis=-1, keepdims=True)
    return centred * lax.rsqrt(variance + 1e-05) * gain + shift


def kernel(
    bands,
    feat_hbm,
    corners_hbm,
    bilinear_hbm,
    attention_hbm,
    w_value_hbm,
    b_value_hbm,
    w_out_hbm,
    b_out_hbm,
    gain1_hbm,
    bias1_hbm,
    w_in_hbm,
    b_in_hbm,
    w_ff_hbm,
    b_ff_hbm,
    gain2_hbm,
    bias2_hbm,
    out,
    gathered,
    corners,
    bilinear,
    attention,
    w_value,
    b_value,
    w_out,
    b_out,
    gain1,
    bias1,
    w_in,
    b_in,
    w_ff,
    b_ff,
    gain2,
    bias2,
    w_value_t,
    shift_t,
    turned_t,
    row_t,
    column_t,
    row_next_t,
    column_next_t,
    place_t,
    weight_t,
    matrix,
    samp_t,
    line_sem,
    across_sem,
    recv_sem,
    cross_sem,
    load_sem,
    late_sem,
):
    rows = [ROWS_DEV // 4**level for level in range(LEVELS)]
    starts = [sum(rows[:level]) for level in range(LEVELS)]
    widths = [MAP_W // 2**level for level in range(LEVELS)]
    tokens, model = feat_hbm.shape
    head_dim = model // HEADS
    padded = matrix.shape[3]
    halves = matrix.shape[2]
    points = HEADS * LEVELS * POINTS
    me = lax.axis_index("band")

    line = bands // 2
    mine_z, mine_y = me // 2, lax.rem(me, 2)
    partner = mine_z * 2 + 1 - mine_y
    cuts = [(begin, min(begin + CHUNK, tokens) - begin) for begin in range(0, tokens, CHUNK)]

    barrier = pltpu.get_barrier_semaphore()

    def greet(target):
        pl.semaphore_signal(barrier, inc=1, device_id={"band": target}, device_id_type=MESH)

    at_start, at_stop = mine_z == 0, mine_z == line - 1
    direct = [(mine_z > 0, me - 2), (mine_z < line - 1, me + 2)]
    greeted = [*direct]
    if line > 2:
        direct.append((at_stop, mine_y))
        greeted.append((at_start, (line - 1) * 2 + mine_y))
    greet(partner)
    for exists, target in greeted:
        pl.when(exists)(functools.partial(greet, target))

    sources = (
        feat_hbm, corners_hbm, bilinear_hbm, attention_hbm, w_value_hbm, b_value_hbm,
        w_out_hbm, b_out_hbm, gain1_hbm, bias1_hbm, w_in_hbm, b_in_hbm, w_ff_hbm, b_ff_hbm,
        gain2_hbm, bias2_hbm,
    )
    targets = (
        gathered.at[me], corners, bilinear, attention, w_value, b_value,
        w_out, b_out, gain1, bias1, w_in, b_in, w_ff, b_ff, gain2, bias2,
    )
    loads = [
        pltpu.make_async_copy(source, target, load_sem.at[number])
        for number, (source, target) in enumerate(zip(sources, targets))
    ]
    for load in loads:
        load.start()

    def move(part, target, send, receive):
        return pltpu.make_async_remote_copy(
            src_ref=part,
            dst_ref=part,
            send_sem=send,
            recv_sem=receive,
            device_id={"band": target},
            device_id_type=MESH,
        )

    def along_line(block, cut, target, way):
        part = gathered.at[block, pl.ds(*cuts[cut])] if cut is not None else gathered.at[block]
        receive = recv_sem.at[block // 2, cut or 0]
        return move(part, target, line_sem.at[way], receive)

    def across(block, cut, way):
        part = gathered.at[block, pl.ds(*cuts[cut])] if cut is not None else gathered.at[block]
        return move(part, partner, across_sem.at[way], cross_sem.at[block // 2])

    both = jnp.minimum(mine_z, line - 1 - mine_z)
    more_right = mine_z * 2 < line

    def arrival(number):
        paired = number <= 2 * both
        from_left = jnp.where(paired, number % 2 == 0, jnp.logical_not(more_right))
        distance = jnp.where(paired, (number + 1) // 2, number - both)
        skipped = line - 1 if number == 2 else max(number - 1, 1)
        distance = jnp.where(at_start, skipped, distance)
        place = mine_z + jnp.where(from_left, -distance, distance)
        onto = jnp.where(from_left, mine_z + 1, mine_z - 1)
        exists = jnp.logical_and(onto >= 0, onto < line)
        if line > 2:
            exists = jnp.logical_and(exists, onto - place != 1 - line)
        return place, exists, onto * 2 + mine_y

    arrivals = [arrival(number) for number in range(1, line)]
    near = [place * 2 + mine_y for place, _, _ in arrivals]
    far = [place * 2 + 1 - mine_y for place, _, _ in arrivals]

    loads[0].wait()
    pl.semaphore_wait(barrier, 1 + sum(exists.astype(jnp.int32) for exists, _ in direct))
    for cut in range(len(cuts)):
        for way in range(2):
            exists, target = direct[way]
            pl.when(exists)(along_line(me, cut, target, way).start)
        across(me, cut, 0).start()
    for cut in range(len(cuts)):
        for way in range(2, len(direct)):
            exists, target = direct[way]
            pl.when(exists)(along_line(me, cut, target, way).start)

    later = pl.ds(cuts[LATE][0], tokens - cuts[LATE][0])
    sooner = pl.ds(0, cuts[LATE][0])
    second = jnp.logical_and(mine_z == 1, line > 2)
    bridge = jnp.logical_and(second, mine_y == 0)

    def across_late(block, part):
        return move(gathered.at[block, part], partner, late_sem.at[0], late_sem.at[1])

    def across_soon(block, way):
        part = gathered.at[block, sooner]
        return move(part, partner, across_sem.at[way], cross_sem.at[block // 2])

    def bridged(block):
        part = gathered.at[block, later]
        return move(part, me - 2, late_sem.at[2], cross_sem.at[block // 2])

    def spared(number):
        return jnp.logical_and(me == 1, near[number] // 2 == 2)

    def forward(number, cut):
        block = near[number]
        _, exists, target = arrivals[number]
        copy = along_line(block, cut, target, len(direct) + number)
        copy.wait_recv()
        pl.when(exists)(copy.start)
        if cut < LATE:
            across(block, cut, 1 + number).start()
        elif number == 0:
            pl.when(second)(across_late(block, pl.ds(*cuts[cut])).start)
            pl.when(jnp.logical_not(second))(across(block, cut, 1 + number).start)
        else:
            pl.when(jnp.logical_not(spared(number)))(across(block, cut, 1 + number).start)

    for load in loads[1:6]:
        load.wait()
    w_value_t[...] = jnp.transpose(w_value[...].astype(F32)).astype(BF16)
    shift_t[...] = jnp.transpose(jnp.broadcast_to(b_value[...], (LANES, model)))

    def turned(block):
        tail = jnp.zeros((padded - tokens, block.shape[1]), F32)
        table = jnp.transpose(jnp.concatenate([block, tail], axis=0))
        return [table[:, half * LANES : (half + 1) * LANES] for half in range(halves)]

    for half, table in enumerate(turned(corners[...].astype(F32))):
        turned_t[half] = table
    level_of = lax.broadcasted_iota(jnp.int32, (points, LANES), 0) // POINTS % LEVELS
    width_of = jnp.where(level_of == 0, float(widths[0]), float(widths[1]))
    inverse = jnp.where(level_of == 0, 1.0 / widths[0], 1.0 / widths[1])
    for half in range(halves):
        place = turned_t[half, pl.ds(0, points, stride=4), :]
        place_t[half] = place
        row = jnp.floor((place + 0.5) * inverse)
        row_t[half] = row
        column_t[half] = place - row * width_of
        row = jnp.floor((place + 1.5) * inverse)
        row_next_t[half] = row
        column_next_t[half] = place + 1.0 - row * width_of
    for half, table in enumerate(turned(bilinear[...])):
        turned_t[half] = table
    for half, share in enumerate(turned(attention[...])):
        for corner in range(4):
            product = share * turned_t[half, pl.ds(corner, points, stride=4), :]
            weight_t[corner, half] = product.astype(BF16).astype(F32)
    samp_t[...] = jnp.zeros(samp_t.shape, F32)

    iota = lax.broadcasted_iota(jnp.int32, (UNIT, LANES), 0).astype(F32)
    zero = jnp.zeros((UNIT, LANES), BF16)

    def spread(table, *at):
        *lead, point = at
        return jnp.broadcast_to(table[(*lead, pl.ds(point, 1), slice(None))], (UNIT, LANES))

    def build(piece, carry):
        head, half = piece // halves, piece % halves
        for level in (0, 1):
            width, count = widths[level], rows[level]
            total = count * bands // width
            base = (head * LEVELS + level) * POINTS
            spans = min(width, 4 * UNIT)
            own_row = [spread(row_t, half, base + which).astype(BF16) for which in range(POINTS)]
            own_column = [
                spread(column_t, half, base + which).astype(BF16) for which in range(POINTS)
            ]
            next_row = [
                spread(row_next_t, half, base + which).astype(BF16) for which in range(POINTS)
            ]
            next_column = [
                spread(column_next_t, half, base + which).astype(BF16) for which in range(POINTS)
            ]
            weight = [
                [spread(weight_t, corner, half, base + which).astype(BF16) for corner in range(4)]
                for which in range(POINTS)
            ]
            for first in range(0, width, spans):
                top, bottom = [], []
                for unit in range(first, first + spans, UNIT):
                    at = (iota + float(unit)).astype(BF16)
                    for which in range(POINTS):
                        left = at == own_column[which]
                        right = at == next_column[which]
                        w = weight[which]
                        top.append(jnp.where(left, w[0], jnp.where(right, w[1], zero)))
                        bottom.append(jnp.where(left, w[2], jnp.where(right, w[3], zero)))
                before = None
                for row in range(total):
                    now = [value == float(row) for value in own_row]
                    turn = [value == float(row) for value in next_row] if first == 0 else now
                    for number in range(spans // UNIT):
                        masks = turn if number == 0 else now
                        earlier = None if before is None else before[0 if number == 0 else 1]
                        entry = None
                        for which in range(POINTS):
                            index = number * POINTS + which
                            under = (
                                zero
                                if earlier is None
                                else jnp.where(earlier[which], bottom[index], zero)
                            )
                            term = jnp.where(masks[which], top[index], under)
                            entry = term if entry is None else entry + term
                        place = row * width + first + number * UNIT
                        block, inside = place // count, starts[level] + place % count
                        matrix[block, head, half, inside : inside + UNIT, :] = entry
                    before = (turn, now)
        exact = max(rows[2], rows[3]) * bands <= 256
        kind = BF16 if exact else F32
        begin = padded - UNIT
        row_at = iota + float(begin)
        third = row_at < float(starts[3])
        valid = row_at < float(starts[3] + rows[3])
        unit_zero = jnp.zeros((UNIT, LANES), kind)

        def mixed(table, *at):
            pair = [
                spread(table, *at, (head * LEVELS + level) * POINTS + which) for level in (2, 3)
            ]
            return jnp.where(third, pair[0], pair[1]).astype(kind)

        coarse = []
        for which in range(POINTS):
            coarse.append(
                (
                    mixed(place_t, half),
                    [mixed(weight_t, corner, half) for corner in range(4)],
                )
            )
        for block in range(bands):
            position = jnp.where(
                third,
                row_at + float(block * rows[2] - starts[2]),
                jnp.where(valid, row_at + float(block * rows[3] - starts[3]), -1000.0),
            )
            under = position - jnp.where(third, float(widths[2]), float(widths[3]))
            spots = [
                spot.astype(kind) for spot in (position, position - 1.0, under, under - 1.0)
            ]
            entry = None
            for place, weights in coarse:
                term = unit_zero
                for spot, weight in zip(spots, weights):
                    term = jnp.where(spot == place, weight, term)
                entry = term if entry is None else entry + term
            matrix[block, head, half, begin:padded, :] = entry.astype(BF16)
        return carry

    lane = lax.broadcasted_iota(jnp.int32, (model, LANES), 1)

    def consume(block):
        value_t = lax.dot_general(
            w_value_t[...], gathered[block], (((1,), (1,)), ((), ())), preferred_element_type=F32
        )
        pieces = []
        for half in range(halves):
            stop = min(tokens, (half + 1) * LANES)
            part = value_t[:, half * LANES : stop]
            count = stop - half * LANES
            if count < LANES:
                part = jnp.concatenate(
                    [part, jnp.zeros((model, LANES - count), F32)], axis=1
                )
            part = part + shift_t[...]
            if count < LANES:
                part = jnp.where(lane < count, part, 0.0)
            pieces.append(part.astype(BF16))
        value = jnp.concatenate(pieces, axis=1)
        for head in range(HEADS):
            into = slice(head * head_dim, (head + 1) * head_dim)
            lookup = jnp.concatenate([matrix[block, head, half] for half in range(halves)], axis=1)
            samp_t[into, :] += jnp.dot(value[into, :], lookup, preferred_element_type=F32)

    def consume_across(block):
        across(block, None, 0).wait_recv()
        consume(block)

    def consume_first_across():
        block = far[0]
        pl.when(jnp.logical_not(second))(across(block, None, 0).wait_recv)
        pl.when(second)(across_soon(block, 0).wait_recv)
        pl.when(jnp.logical_and(second, mine_y == 1))(across_late(block, later).wait_recv)
        consume(block)

    everything = HEADS * halves
    done = 0
    for index, (cut, number) in enumerate(
        (cut, number) for number in range(line - 1) for cut in range(len(cuts))
    ):
        upto = min(everything, AHEAD + index)
        if upto > done:
            lax.fori_loop(done, upto, build, 0)
            done = upto
        if number == 2 and cut == 0:

            @pl.when(bridge)
            def _():
                across_late(far[0], later).wait_recv()
                bridged(far[0]).start()

        forward(number, cut)
    if done < everything:
        lax.fori_loop(done, everything, build, 0)
    consume(me)
    consume_across(partner)
    for number in range(line - 1):
        consume(near[number])
        if number == 1:
            consume_first_across()
        elif number:
            consume_across(far[number - 1])
    consume_across(far[line - 2])

    for load in loads[6:]:
        load.wait()
    attended = lax.dot_general(
        samp_t[...].astype(BF16), w_out[...], (((0,), (0,)), ((), ())), preferred_element_type=F32
    )[0:tokens, :] + b_out[...]
    middle = norm(gathered[me].astype(F32) + attended, gain1[...], bias1[...]).astype(BF16)
    hidden = jnp.maximum(
        jnp.dot(middle, w_in[...], preferred_element_type=F32) + b_in[...], 0.0
    ).astype(BF16)
    result = (
        middle.astype(F32)
        + jnp.dot(hidden, w_ff[...], preferred_element_type=F32)
        + b_ff[...]
    )
    out[...] = norm(result, gain2[...], bias2[...]).astype(BF16)

    for way, (exists, target) in enumerate(direct):
        pl.when(exists)(along_line(me, None, target, way).wait_send)
    across(me, None, 0).wait_send()
    for number, (_, exists, target) in enumerate(arrivals):
        pl.when(exists)(
            along_line(near[number], None, target, len(direct) + number).wait_send
        )
        short = second if number == 0 else spared(number)
        pl.when(short)(across_soon(near[number], 1 + number).wait_send)
        pl.when(jnp.logical_not(short))(across(near[number], None, 1 + number).wait_send)
    pl.when(second)(across_late(near[0], later).wait_send)
    pl.when(bridge)(bridged(far[0]).wait_send)


def body(bands, *args):
    tokens, model = args[0].shape
    padded = -(-tokens // LANES) * LANES
    halves = padded // LANES
    samples = args[1].shape[1]
    points = samples // 4
    operands = [
        argument.reshape(1, -1) if argument.ndim == 1 else argument for argument in args
    ]
    cuts = -(-tokens // CHUNK)
    table = pltpu.VMEM((halves, points, LANES), F32)
    scratch = [
        pltpu.VMEM((bands, tokens, model), BF16),
        *(pltpu.VMEM(operand.shape, operand.dtype) for operand in operands[1:]),
        pltpu.VMEM(args[4].shape, BF16),
        pltpu.VMEM((model, LANES), F32),
        pltpu.VMEM((halves, samples, LANES), F32),
        table,
        table,
        table,
        table,
        table,
        pltpu.VMEM((4, halves, points, LANES), F32),
        pltpu.VMEM((bands, HEADS, halves, padded, LANES), BF16),
        pltpu.VMEM((model, padded), F32),
        pltpu.SemaphoreType.DMA((2 + bands // 2,)),
        pltpu.SemaphoreType.DMA((bands // 2,)),
        pltpu.SemaphoreType.DMA((bands // 2, cuts)),
        pltpu.SemaphoreType.DMA((bands // 2,)),
        pltpu.SemaphoreType.DMA((len(operands),)),
        pltpu.SemaphoreType.DMA((3,)),
    ]
    held = bands * HEADS * padded * padded * 2 + bands * tokens * model * 2
    limit = held + 16 * 1024 * 1024
    return pl.pallas_call(
        functools.partial(kernel, bands),
        out_shape=jax.ShapeDtypeStruct((tokens, model), BF16),
        in_specs=[pl.BlockSpec(memory_space=pl.ANY)] * len(operands),
        out_specs=pl.BlockSpec(memory_space=pltpu.VMEM),
        scratch_shapes=scratch,
        compiler_params=pltpu.CompilerParams(
            collective_id=0, has_side_effects=True, vmem_limit_bytes=limit
        ),
        name="layer",
    )(*(pltpu.with_memory_space_constraint(operand, pltpu.HBM) for operand in operands))


def solution(mesh):
    split = P(("dp", "band"), None)
    in_specs = (split,) * 4 + (P(),) * 12
    return jax.shard_map(
        functools.partial(body, mesh.shape["band"]),
        mesh=mesh,
        in_specs=in_specs,
        out_specs=split,
        check_vma=False,
    )
```
